32 devices in a mesh: section: 2 (over core), row: 4 (over y, x), col: 4 (over z).
Axes of the slice: x: 2, y: 2, z: 4, core: 2. Of those that a mesh axis runs over, the one named last changes fastest.
Arguments:
- section_inputs: bfloat16 [2, 2, 48, 4096], P('section', None, 'col', 'row'), may hold values from -6 to 6
- out_grad: bfloat16 [2, 48, 4096], P(None, 'col', 'row'), may hold values from -6 to 6
- gate_weight: bfloat16 [2, 4096, 14336], P('section', 'row', 'col'), may hold values from -0.09375 to 0.09375
- up_weight: bfloat16 [2, 4096, 14336], P('section', 'row', 'col'), may hold values from -0.09375 to 0.09375
- down_weight: bfloat16 [2, 14336, 4096], P('section', 'col', 'row'), may hold values from -0.046875 to 0.046875
Outputs:
- input_grads: bfloat16 [2, 2, 48, 4096], P('section', None, 'col', 'row')
- grad_gate: float32 [2, 4096, 14336], P('section', 'row', 'col')
- grad_up: float32 [2, 4096, 14336], P('section', 'row', 'col')
- grad_down: float32 [2, 14336, 4096], P('section', 'col', 'row')
The draws below stay inside these ranges and needn't reach their ends.
All inputs are finite; a program needn't handle non-finite values.
Results may differ from the reference program's by a relative error of at most 0.025.
Values may be sent and summed in bfloat16 or wider, within the bound.
No kernel may reach another device: no remote copies, remote signals or barrier semaphores. Data moves between devices by JAX's collectives and lax.ppermute only.
A program may use at most 192 MiB of HBM per device.

```python
import jax
import jax.numpy as jnp

D = 4096
FF = 14336
MICRO = 2
SECTIONS = 2
TOKENS = 48
N_ROW = 4


def level_of(own_key, shape, pieces, low, top_value):
    gain, own = 1.0, jax.random.fold_in(own_key, 6)
    for position, shards_of in pieces:
        steps = jnp.exp(jax.random.uniform(jax.random.fold_in(own, position), (shards_of,), jnp.float32, low / len(pieces), top_value / len(pieces)))
        gain = gain * jnp.repeat(steps, shape[position] // shards_of).reshape([-1 if axis == position else 1 for axis in range(len(shape))])
    return gain


def gaussian(own_key, extent, scale, most, cuts=(), dtype=jnp.bfloat16):
    result = scale * jax.random.normal(own_key, extent, jnp.float32)
    if cuts:
        result = result * level_of(own_key, extent, cuts, -0.22, 0.18)
    return jnp.clip(result, -most, most).astype(dtype)


def setup_inputs(seed: int = 0) -> dict:
    arg_keys = jax.random.split(jax.random.key(seed), 6)
    section_inputs = gaussian(arg_keys[0], (SECTIONS, MICRO, TOKENS, D), 1.0, 6.0, ((0, 2), (2, 4), (3, 4)))
    out_grad = gaussian(arg_keys[1], (MICRO, TOKENS, D), 1.0, 6.0, ((1, 4), (2, 4)))
    gate_weight = gaussian(arg_keys[2], (SECTIONS, D, FF), D ** -0.5, 0.09375, ((0, 2), (1, 4), (2, 4)))
    up_weight = gaussian(arg_keys[3], (SECTIONS, D, FF), D ** -0.5, 0.09375, ((0, 2), (1, 4), (2, 4)))
    down_weight = gaussian(arg_keys[4], (SECTIONS, FF, D), FF ** -0.5, 0.046875, ((0, 2), (1, 4), (2, 4)))
    return dict(section_inputs=section_inputs, out_grad=out_grad, gate_weight=gate_weight, up_weight=up_weight, down_weight=down_weight)


def blocked_sum(left, right):
    width = D // N_ROW
    total = jnp.zeros((left.shape[0], right.shape[1]), jnp.float32)
    for block in range(N_ROW):
        piece = jnp.dot(left[:, block * width:(block + 1) * width], right[block * width:(block + 1) * width],
                        preferred_element_type=jnp.float32).astype(jnp.bfloat16)
        total = total + piece.astype(jnp.float32)
    return total


def layer_backward(x_rows, dy_rows, w_gate, w_up, w_down):
    gate_sum = blocked_sum(x_rows, w_gate)
    up_sum = blocked_sum(x_rows, w_up)
    sigmoid_gate = jax.nn.sigmoid(gate_sum)
    activated = gate_sum * sigmoid_gate
    slope = sigmoid_gate * (1.0 + gate_sum * (1.0 - sigmoid_gate))
    hidden = (activated * up_sum).astype(jnp.bfloat16)
    hidden_grad = blocked_sum(dy_rows, w_down.T)
    gate_grad = (hidden_grad * up_sum * slope).astype(jnp.bfloat16)
    up_grad = (hidden_grad * activated).astype(jnp.bfloat16)
    branch = jnp.dot(gate_grad, w_gate.T, preferred_element_type=jnp.float32)
    branch = branch + jnp.dot(up_grad, w_up.T, preferred_element_type=jnp.float32)
    input_grad = (dy_rows.astype(jnp.float32) + branch).astype(jnp.bfloat16)
    gate_update = jnp.dot(x_rows.T, gate_grad, preferred_element_type=jnp.float32)
    up_update = jnp.dot(x_rows.T, up_grad, preferred_element_type=jnp.float32)
    down_update = jnp.dot(hidden.T, dy_rows, preferred_element_type=jnp.float32)
    return input_grad, gate_update, up_update, down_update


def reference(section_inputs, out_grad, gate_weight, up_weight, down_weight):
    carried = [out_grad[micro_index] for micro_index in range(MICRO)]
    input_list = []
    gate_list = []
    up_list = []
    down_list = []
    for section_number in reversed(range(SECTIONS)):
        gate_total = jnp.zeros((D, FF), jnp.float32)
        up_total = jnp.zeros((D, FF), jnp.float32)
        down_total = jnp.zeros((FF, D), jnp.float32)
        produced = []
        for micro_index in range(MICRO):
            input_grad, gate_update, up_update, down_update = layer_backward(
                section_inputs[section_number, micro_index], carried[micro_index],
                gate_weight[section_number], up_weight[section_number], down_weight[section_number])
            produced.append(input_grad)
            gate_total = gate_total + gate_update
            up_total = up_total + up_update
            down_total = down_total + down_update
        carried = produced
        input_list.insert(0, jnp.stack(produced))
        gate_list.insert(0, gate_total)
        up_list.insert(0, up_total)
        down_list.insert(0, down_total)
    return jnp.stack(input_list), jnp.stack(gate_list), jnp.stack(up_list), jnp.stack(down_list)
```

```python
import functools

import jax
import jax.numpy as jnp
from jax import lax
from jax.experimental import pallas as pl
from jax.experimental.pallas import tpu as pltpu
from jax.sharding import PartitionSpec as P


NN = (((1,), (0,)), ((), ()))
NT = (((1,), (1,)), ((), ()))
TN = (((0,), (0,)), ((), ()))
BF16 = jnp.bfloat16
F32 = jnp.float32
VMEM_LIMIT = 48 * 1024 * 1024


def mm(left, right, dims):
    return lax.dot_general(left, right, dims, preferred_element_type=F32)


def cost(flops, *moved):
    total = sum(x.size * x.dtype.itemsize for x in moved)
    return pl.CostEstimate(flops=flops, bytes_accessed=total, transcendentals=0)


def aligned(width):
    return width % 128 == 0


def whole_block(shape):
    return pl.BlockSpec(shape, lambda *_: (0,) * len(shape))


def parts_kernel(dims, count, row_ref, act_ref, w_ref, *out_refs):
    k = pl.program_id(0)
    result = mm(act_ref[...], w_ref[...], dims).astype(BF16)
    for j in range(count):
        @pl.when(k == j)
        def _():
            out_refs[j][...] = result


def partial_parts(act, w, my_row, n_row, transposed):
    dims = NT if transposed else NN
    hidden_axis = 0 if transposed else 1
    width = w.shape[hidden_axis] // n_row
    if not aligned(width):
        full = mm(act, w, dims).astype(BF16)
        return [lax.dynamic_slice_in_dim(full, (my_row ^ k) * width, width, 1) for k in range(n_row)]
    if transposed:
        w_spec = pl.BlockSpec((width, w.shape[1]), lambda k, r: (r[0] ^ k, 0))
    else:
        w_spec = pl.BlockSpec((w.shape[0], width), lambda k, r: (0, r[0] ^ k))
    part = jax.ShapeDtypeStruct((act.shape[0], width), BF16)
    return pl.pallas_call(
        functools.partial(parts_kernel, dims, n_row),
        grid_spec=pltpu.PrefetchScalarGridSpec(
            num_scalar_prefetch=1,
            grid=(n_row,),
            in_specs=[whole_block(act.shape), w_spec],
            out_specs=[whole_block(part.shape)] * n_row,
        ),
        out_shape=[part] * n_row,
        compiler_params=pltpu.CompilerParams(vmem_limit_bytes=VMEM_LIMIT),
        cost_estimate=cost(2 * act.shape[0] * w.size, act, w),
        name="partial_parts",
    )(my_row.reshape(1), act, w)


def branch_kernel(count, pieces, row_ref, *refs):
    gates, ups = refs[:count], refs[count:2 * count]
    wg_ref, wu_ref = refs[2 * count:2 * count + 2]
    outs = refs[2 * count + 2:2 * count + 2 + pieces]
    acc_ref = refs[-1]
    k = pl.program_id(0)
    for j in range(count):
        @pl.when(k == j)
        def _():
            value = mm(gates[j][...], wg_ref[...], NT) + mm(ups[j][...], wu_ref[...], NT)
            acc_ref[...] = value if j == 0 else acc_ref[...] + value

    @pl.when(k == count - 1)
    def _():
        rows = acc_ref.shape[0] // pieces
        for j in range(pieces):
            outs[j][...] = acc_ref[j * rows:(j + 1) * rows, :].astype(BF16)


def branch_parts(gates, ups, w_gate, w_up, my_row, n_row, n_col):
    tokens, width = gates[0].shape
    rows = tokens // n_col
    if not aligned(width):
        place = lambda parts: gather_parts(parts, my_row)
        full = mm(place(gates), w_gate, NT) + mm(place(ups), w_up, NT)
        full = full.astype(BF16)
        return [full[j * rows:(j + 1) * rows] for j in range(n_col)]
    part = jax.ShapeDtypeStruct((rows, w_gate.shape[0]), BF16)
    w_spec = pl.BlockSpec((w_gate.shape[0], width), lambda k, r: (0, r[0] ^ k))
    return pl.pallas_call(
        functools.partial(branch_kernel, n_row, n_col),
        grid_spec=pltpu.PrefetchScalarGridSpec(
            num_scalar_prefetch=1,
            grid=(n_row,),
            in_specs=[whole_block((tokens, width))] * (2 * n_row) + [w_spec, w_spec],
            out_specs=[whole_block(part.shape)] * n_col,
            scratch_shapes=[pltpu.VMEM((tokens, w_gate.shape[0]), F32)],
        ),
        out_shape=[part] * n_col,
        compiler_params=pltpu.CompilerParams(vmem_limit_bytes=VMEM_LIMIT),
        cost_estimate=cost(4 * tokens * w_gate.size, w_gate, w_up),
        name="branch_parts",
    )(my_row.reshape(1), *gates, *ups, w_gate, w_up)


def gather_parts(parts, my_row):
    order = my_row ^ jnp.arange(len(parts))
    return jnp.concatenate(list(jnp.stack(parts)[order]), axis=1)


def grad_kernel(count, hidden_first, info_ref, act_ref, *refs):
    news, olds, out_ref = refs[:count], refs[count:2 * count], refs[-1]
    k = pl.program_id(0)
    fresh = info_ref[1] == 1

    def run(part_ref):
        if hidden_first:
            out_ref[...] = mm(part_ref[...], act_ref[...], TN)
        else:
            out_ref[...] = mm(act_ref[...], part_ref[...], TN)

    for j in range(count):
        @pl.when((k == j) & fresh)
        def _():
            run(news[j])

        @pl.when((k == j) & jnp.logical_not(fresh))
        def _():
            run(olds[j])


def weight_grad(act, news, olds, my_row, is_fresh, hidden_first, name):
    count = len(news)
    tokens, width = news[0].shape
    features = act.shape[1]
    if not aligned(width):
        hidden = gather_parts([jnp.where(is_fresh, a, b) for a, b in zip(news, olds)], my_row)
        return mm(hidden, act, TN) if hidden_first else mm(act, hidden, TN)
    if hidden_first:
        out = jax.ShapeDtypeStruct((width * count, features), F32)
        out_spec = pl.BlockSpec((width, features), lambda k, r: (r[0] ^ k, 0))
    else:
        out = jax.ShapeDtypeStruct((features, width * count), F32)
        out_spec = pl.BlockSpec((features, width), lambda k, r: (0, r[0] ^ k))
    info = jnp.stack([my_row, is_fresh.astype(jnp.int32)])
    return pl.pallas_call(
        functools.partial(grad_kernel, count, hidden_first),
        grid_spec=pltpu.PrefetchScalarGridSpec(
            num_scalar_prefetch=1,
            grid=(count,),
            in_specs=[whole_block(act.shape)] + [whole_block((tokens, width))] * (2 * count),
            out_specs=out_spec,
        ),
        out_shape=out,
        compiler_params=pltpu.CompilerParams(vmem_limit_bytes=VMEM_LIMIT),
        cost_estimate=cost(2 * tokens * features * width * count, out),
        name=name,
    )(info, act, *news, *olds)


def row_swap(block, k, sections):
    n_row = lax.axis_size("row")
    pairs = [(s * n_row + i, s * n_row + (i ^ k)) for s in sections for i in range(n_row)]
    return lax.ppermute(block, ("section", "row"), pairs)


def col_shift(block, k, routes):
    n_col = lax.axis_size("col")
    pairs = [
        (source * n_col + i, target * n_col + (i + k) % n_col)
        for source, target in routes
        for i in range(n_col)
    ]
    return lax.ppermute(block, ("section", "col"), pairs)


def row_sum(parts, section):
    arrived = [parts[0]] + [row_swap(parts[k], k, [section]) for k in range(1, len(parts))]
    return sum(block.astype(F32) for block in arrived)


def row_spread(own, section):
    return [own] + [row_swap(own, k, [section]) for k in range(1, lax.axis_size("row"))]


def shards(section_inputs, out_grad, gate_weight, up_weight, down_weight):
    section_id = lax.axis_index("section")
    my_row = lax.axis_index("row").astype(jnp.int32)
    n_sections, n_row, n_col = (lax.axis_size(a) for a in ("section", "row", "col"))
    everyone = [(s, s) for s in range(n_sections)]
    w_gate, w_up, w_down = gate_weight[0], up_weight[0], down_weight[0]
    merged_shape = (section_inputs.shape[1] * section_inputs.shape[2], section_inputs.shape[3])
    x_local = section_inputs[0].reshape(merged_shape)
    dy_local = out_grad.reshape(merged_shape)
    last = n_sections - 1

    dy_whole = jnp.concatenate(
        [dy_local] + [col_shift(dy_local, k, [(last, last)]) for k in range(1, n_col)], axis=0)
    x_whole = jnp.concatenate(
        [x_local] + [col_shift(x_local, k, everyone) for k in range(1, n_col)], axis=0)
    gate_parts = partial_parts(x_whole, w_gate, my_row, n_row, False)
    up_parts = partial_parts(x_whole, w_up, my_row, n_row, False)

    input_grad = dy_local
    result = None
    olds = None
    for step in range(n_sections):
        active = last - step
        is_active = section_id == active
        if step:
            arrived = [col_shift(input_grad, k, [(active + 1, active)]) for k in range(n_col)]
            dy_local = jnp.where(is_active, arrived[0], dy_local)
            dy_whole = jnp.where(is_active, jnp.concatenate(arrived, axis=0), dy_whole)
        down_parts = partial_parts(dy_whole, w_down, my_row, n_row, True)
        gate = row_sum(gate_parts, active)
        up = row_sum(up_parts, active)
        hidden_grad = row_sum(down_parts, active)
        sigmoid_gate = jax.nn.sigmoid(gate)
        activated = gate * sigmoid_gate
        slope = sigmoid_gate * (1.0 + gate * (1.0 - sigmoid_gate))
        hidden = (activated * up).astype(BF16)
        gate_grad = (hidden_grad * up * slope).astype(BF16)
        up_grad = (hidden_grad * activated).astype(BF16)
        gates = row_spread(gate_grad, active)
        ups = row_spread(up_grad, active)
        hiddens = row_spread(hidden, active)
        pieces = branch_parts(gates, ups, w_gate, w_up, my_row, n_row, n_col)
        total = pieces[0].astype(F32)
        for k in range(1, n_col):
            total = total + col_shift(pieces[k], -k, [(active, active)]).astype(F32)
        input_grad = (dy_local.astype(F32) + total).astype(BF16)
        result = input_grad if result is None else jnp.where(is_active, input_grad, result)
        news = (gates, ups, hiddens)
        if step == last:
            olds = news if olds is None else olds
        elif olds is None:
            olds = news
        else:
            olds = jax.tree.map(functools.partial(jnp.where, is_active), news, olds)

    is_fresh = section_id == 0
    grad_down = weight_grad(dy_whole, news[2], olds[2], my_row, is_fresh, True, "grad_down")
    grad_gate = weight_grad(x_whole, news[0], olds[0], my_row, is_fresh, False, "grad_gate")
    grad_up = weight_grad(x_whole, news[1], olds[1], my_row, is_fresh, False, "grad_up")
    return (
        result.reshape(section_inputs.shape),
        grad_gate[None],
        grad_up[None],
        grad_down[None],
    )


def solution(mesh):
    return jax.shard_map(
        shards,
        mesh=mesh,
        in_specs=(
            P("section", None, "col", "row"),
            P(None, "col", "row"),
            P("section", "row", "col"),
            P("section", "row", "col"),
            P("section", "col", "row"),
        ),
        out_specs=(
            P("section", None, "col", "row"),
            P("section", "row", "col"),
            P("section", "row", "col"),
            P("section", "col", "row"),
        ),
        check_vma=False,
    )
```

```python
import functools

import jax
import jax.numpy as jnp
from jax import lax
from jax.experimental import pallas as pl
from jax.experimental.pallas import tpu as pltpu
from jax.sharding import PartitionSpec as P


NN = (((1,), (0,)), ((), ()))
NT = (((1,), (1,)), ((), ()))
TN = (((0,), (0,)), ((), ()))
BF16 = jnp.bfloat16
F32 = jnp.float32
VMEM_LIMIT = 48 * 1024 * 1024
SPLIT = 2


def mm(left, right, dims):
    return lax.dot_general(left, right, dims, preferred_element_type=F32)


def cost(flops, *moved):
    total = sum(x.size * x.dtype.itemsize for x in moved)
    return pl.CostEstimate(flops=flops, bytes_accessed=total, transcendentals=0)


def use_kernels(width, features):
    return width % 128 == 0 and features % (128 * SPLIT) == 0


def whole_block(shape):
    return pl.BlockSpec(shape, lambda *_: (0,) * len(shape))


def place(parts, my_row):
    order = my_row ^ jnp.arange(len(parts))
    return jnp.concatenate(list(jnp.stack(parts)[order]), axis=1)


def params():
    return pltpu.CompilerParams(vmem_limit_bytes=VMEM_LIMIT)


def parts_kernel(dims, count, weights, row_ref, act_ref, *refs):
    w_refs, out_refs, acc_ref = refs[:weights], refs[weights:weights + count], refs[-1]
    k, h = pl.program_id(0), pl.program_id(1)
    act = act_ref[...]
    values = [mm(act, w[...], dims) for w in w_refs]
    width = values[0].shape[1]
    for t, value in enumerate(values):
        @pl.when(h == 0)
        def _():
            acc_ref[t] = value

        @pl.when((h > 0) & (h < SPLIT - 1))
        def _():
            acc_ref[t] += value

        @pl.when(h == SPLIT - 1)
        def _():
            total = (acc_ref[t] + value).astype(BF16)
            for j in range(count):
                @pl.when(k == j)
                def _():
                    out_refs[j][:, t * width:(t + 1) * width] = total


def partial_parts(act, ws, my_row, n_row, transposed):
    dims = NT if transposed else NN
    hidden_axis = 0 if transposed else 1
    width = ws[0].shape[hidden_axis] // n_row
    tokens, features = act.shape
    if not use_kernels(width, features):
        fulls = [mm(act, w, dims).astype(BF16) for w in ws]
        return [
            jnp.concatenate(
                [lax.dynamic_slice_in_dim(f, (my_row ^ k) * width, width, 1) for f in fulls], axis=1)
            for k in range(n_row)
        ]
    piece = features // SPLIT
    if transposed:
        w_spec = pl.BlockSpec((width, piece), lambda k, h, r: (r[0] ^ k, h))
    else:
        w_spec = pl.BlockSpec((piece, width), lambda k, h, r: (h, r[0] ^ k))
    part = jax.ShapeDtypeStruct((tokens, width * len(ws)), BF16)
    return pl.pallas_call(
        functools.partial(parts_kernel, dims, n_row, len(ws)),
        grid_spec=pltpu.PrefetchScalarGridSpec(
            num_scalar_prefetch=1,
            grid=(n_row, SPLIT),
            in_specs=[pl.BlockSpec((tokens, piece), lambda k, h, r: (0, h))] + [w_spec] * len(ws),
            out_specs=[whole_block(part.shape)] * n_row,
            scratch_shapes=[pltpu.VMEM((len(ws), tokens, width), F32)],
        ),
        out_shape=[part] * n_row,
        compiler_params=params(),
        cost_estimate=cost(2 * tokens * ws[0].size * len(ws), act, *ws),
        name="partial_parts",
    )(my_row.reshape(1), act, *ws)


def branch_kernel(count, pieces, row_ref, *refs):
    grads, (wg_ref, wu_ref) = refs[:count], refs[count:count + 2]
    outs, acc_ref = refs[count + 2:count + 2 + pieces], refs[-1]
    k, h = pl.program_id(0), pl.program_id(1)
    width = wg_ref.shape[1]
    for j in range(count):
        @pl.when(k == j)
        def _():
            value = mm(grads[j][:, :width], wg_ref[...], NT) + mm(grads[j][:, width:], wu_ref[...], NT)
            acc_ref[h] = value if j == 0 else acc_ref[h] + value

    @pl.when(k == count - 1)
    def _():
        rows = acc_ref.shape[1] // pieces
        cols = acc_ref.shape[2]
        for i in range(SPLIT):
            @pl.when(h == i)
            def _():
                for j in range(pieces):
                    outs[j][:, i * cols:(i + 1) * cols] = (
                        acc_ref[i, j * rows:(j + 1) * rows, :].astype(BF16))


def branch_parts(grads, w_gate, w_up, my_row, n_row, n_col):
    tokens, width = grads[0].shape[0], grads[0].shape[1] // 2
    rows, features = tokens // n_col, w_gate.shape[0]
    if not use_kernels(width, features):
        full = mm(place([g[:, :width] for g in grads], my_row), w_gate, NT)
        full = full + mm(place([g[:, width:] for g in grads], my_row), w_up, NT)
        full = full.astype(BF16)
        return [full[j * rows:(j + 1) * rows] for j in range(n_col)]
    part = jax.ShapeDtypeStruct((rows, features), BF16)
    piece = features // SPLIT
    w_spec = pl.BlockSpec((piece, width), lambda k, h, r: (h, r[0] ^ k))
    return pl.pallas_call(
        functools.partial(branch_kernel, n_row, n_col),
        grid_spec=pltpu.PrefetchScalarGridSpec(
            num_scalar_prefetch=1,
            grid=(n_row, SPLIT),
            in_specs=[whole_block(grads[0].shape)] * n_row + [w_spec, w_spec],
            out_specs=[whole_block(part.shape)] * n_col,
            scratch_shapes=[pltpu.VMEM((SPLIT, tokens, piece), F32)],
        ),
        out_shape=[part] * n_col,
        compiler_params=params(),
        cost_estimate=cost(4 * tokens * w_gate.size, w_gate, w_up),
        name="branch_parts",
    )(my_row.reshape(1), *grads, w_gate, w_up)


def grad_kernel(count, hidden_first, info_ref, act_ref, *refs):
    news, olds, out_ref = refs[:count], refs[count:-1], refs[-1]
    k = pl.program_id(0)

    def run(part_ref):
        if hidden_first:
            out_ref[...] = mm(part_ref[...], act_ref[...], TN)
        else:
            out_ref[...] = mm(act_ref[...], part_ref[...], TN)

    for j in range(count):
        if not olds:
            pl.when(k == j)(functools.partial(run, news[j]))
        else:
            fresh = info_ref[1] == 1
            pl.when((k == j) & fresh)(functools.partial(run, news[j]))
            pl.when((k == j) & jnp.logical_not(fresh))(functools.partial(run, olds[j]))


def weight_grad(act, news, olds, my_row, is_fresh, slot, slots, hidden_first, name):
    count = len(news)
    tokens, width = news[0].shape[0], news[0].shape[1] // slots
    features = act.shape[1]
    if not use_kernels(width, features):
        if olds:
            news = [jnp.where(is_fresh, a, b) for a, b in zip(news, olds)]
        hidden = place([a[:, slot * width:(slot + 1) * width] for a in news], my_row)
        return mm(hidden, act, TN) if hidden_first else mm(act, hidden, TN)
    piece = features // SPLIT
    if hidden_first:
        out = jax.ShapeDtypeStruct((width * count, features), F32)
        out_spec = pl.BlockSpec((width, piece), lambda k, h, r: (r[0] ^ k, h))
    else:
        out = jax.ShapeDtypeStruct((features, width * count), F32)
        out_spec = pl.BlockSpec((piece, width), lambda k, h, r: (h, r[0] ^ k))
    info = jnp.stack([my_row, is_fresh.astype(jnp.int32)])
    part_spec = pl.BlockSpec((tokens, width), lambda k, h, r: (0, slot))
    return pl.pallas_call(
        functools.partial(grad_kernel, count, hidden_first),
        grid_spec=pltpu.PrefetchScalarGridSpec(
            num_scalar_prefetch=1,
            grid=(count, SPLIT),
            in_specs=[pl.BlockSpec((tokens, piece), lambda k, h, r: (0, h))]
            + [part_spec] * (count + len(olds)),
            out_specs=out_spec,
        ),
        out_shape=out,
        compiler_params=params(),
        cost_estimate=cost(2 * tokens * features * width * count, out),
        name=name,
    )(info, act, *news, *olds)


def row_swap(block, k, sections):
    n_row = lax.axis_size("row")
    pairs = [(s * n_row + i, s * n_row + (i ^ k)) for s in sections for i in range(n_row)]
    return lax.ppermute(block, ("section", "row"), pairs)


def col_shift(block, k, section_step=0):
    n_sections, n_col = lax.axis_size("section"), lax.axis_size("col")
    pairs = [
        (s * n_col + i, (s + section_step) % n_sections * n_col + (i + k) % n_col)
        for s in range(n_sections)
        for i in range(n_col)
    ]
    return lax.ppermute(block, ("section", "col"), pairs)


def row_collect(parts, sections):
    return [parts[0]] + [row_swap(parts[k], k, sections) for k in range(1, len(parts))]


def row_spread(own, sections):
    return [own] + [row_swap(own, k, sections) for k in range(1, lax.axis_size("row"))]


def total_of(blocks):
    return sum(block.astype(F32) for block in blocks)


def shards(section_inputs, out_grad, gate_weight, up_weight, down_weight):
    section_id = lax.axis_index("section")
    my_row = lax.axis_index("row").astype(jnp.int32)
    n_sections, n_row, n_col = (lax.axis_size(a) for a in ("section", "row", "col"))
    everyone = range(n_sections)
    w_gate, w_up, w_down = gate_weight[0], up_weight[0], down_weight[0]
    merged_shape = (section_inputs.shape[1] * section_inputs.shape[2], section_inputs.shape[3])
    features = merged_shape[1]
    x_local = section_inputs[0].reshape(merged_shape)
    dy_local = out_grad.reshape(merged_shape)
    last = n_sections - 1
    is_fresh = section_id == 0

    pair = jnp.concatenate([x_local, dy_local], axis=1)
    both = jnp.concatenate([pair] + [col_shift(pair, k) for k in range(1, n_col)], axis=0)
    x_whole, dy_whole = both[:, :features], both[:, features:]
    wide_parts = partial_parts(x_whole, [w_gate, w_up], my_row, n_row, False)
    wide = row_collect(wide_parts, everyone)
    width = wide[0].shape[1] // 2
    gate = total_of([w[:, :width] for w in wide])
    up = total_of([w[:, width:] for w in wide])
    sigmoid_gate = jax.nn.sigmoid(gate)
    activated = gate * sigmoid_gate
    slope = sigmoid_gate * (1.0 + gate * (1.0 - sigmoid_gate))
    hidden = (activated * up).astype(BF16)

    input_grad = dy_local
    result = None
    olds = []
    for step in range(n_sections):
        active = last - step
        is_active = section_id == active
        if step:
            arrived = [col_shift(input_grad, k, -1) for k in range(n_col)]
            dy_local = jnp.where(is_active, arrived[0], dy_local)
            dy_whole = jnp.where(is_active, jnp.concatenate(arrived, axis=0), dy_whole)
        down_parts = partial_parts(dy_whole, [w_down], my_row, n_row, True)
        down = row_collect(down_parts, [active] if step == 0 else everyone)
        if step == last:
            grad_down = weight_grad(dy_whole, hiddens, [], my_row, is_fresh, 0, 1, True, "grad_down")
            down, grad_down = lax.optimization_barrier((down, grad_down))
        hidden_grad = total_of(down)
        both_grad = jnp.concatenate(
            [(hidden_grad * up * slope).astype(BF16), (hidden_grad * activated).astype(BF16)], axis=1)
        news = row_spread(both_grad, [active])
        if step == 0:
            hidden, news = lax.optimization_barrier((hidden, news))
            hiddens = row_spread(hidden, everyone)
        pieces = branch_parts(news, w_gate, w_up, my_row, n_row, n_col)
        total = total_of([pieces[0]] + [col_shift(pieces[k], -k) for k in range(1, n_col)])
        input_grad = (dy_local.astype(F32) + total).astype(BF16)
        result = input_grad if result is None else jnp.where(is_active, input_grad, result)
        if step < last:
            olds = [jnp.where(is_active, a, b) for a, b in zip(news, olds)] if olds else news

    grad_gate = weight_grad(x_whole, news, olds, my_row, is_fresh, 0, 2, False, "grad_gate")
    grad_up = weight_grad(x_whole, news, olds, my_row, is_fresh, 1, 2, False, "grad_up")
    return (
        result.reshape(section_inputs.shape),
        grad_gate[None],
        grad_up[None],
        grad_down[None],
    )


def solution(mesh):
    return jax.shard_map(
        shards,
        mesh=mesh,
        in_specs=(
            P("section", None, "col", "row"),
            P(None, "col", "row"),
            P("section", "row", "col"),
            P("section", "row", "col"),
            P("section", "col", "row"),
        ),
        out_specs=(
            P("section", None, "col", "row"),
            P("section", "row", "col"),
            P("section", "row", "col"),
            P("section", "col", "row"),
        ),
        check_vma=False,
    )
```

```python
import functools

import jax
import jax.numpy as jnp
from jax import lax
from jax.experimental import pallas as pl
from jax.experimental.pallas import tpu as pltpu
from jax.sharding import PartitionSpec as P


NN = (((1,), (0,)), ((), ()))
NT = (((1,), (1,)), ((), ()))
TN = (((0,), (0,)), ((), ()))
BF16 = jnp.bfloat16
F32 = jnp.float32
VMEM_LIMIT = 48 * 1024 * 1024
SPLIT = 1


def mm(left, right, dims):
    return lax.dot_general(left, right, dims, preferred_element_type=F32)


def cost(flops, *moved):
    total = sum(x.size * x.dtype.itemsize for x in moved)
    return pl.CostEstimate(flops=flops, bytes_accessed=total, transcendentals=0)


def use_kernels(width, features):
    return width % 128 == 0 and features % (128 * SPLIT) == 0


def whole_block(shape):
    return pl.BlockSpec(shape, lambda *_: (0,) * len(shape))


def place(parts, my_row):
    order = my_row ^ jnp.arange(len(parts))
    return jnp.concatenate(list(jnp.stack(parts)[order]), axis=1)


def params():
    return pltpu.CompilerParams(vmem_limit_bytes=VMEM_LIMIT)


def parts_kernel(dims, count, weights, row_ref, act_ref, *refs):
    w_refs, out_refs, acc_ref = refs[:weights], refs[weights:weights + count], refs[-1]
    k, h = pl.program_id(0), pl.program_id(1)
    act = act_ref[...]
    values = [mm(act, w[...], dims) for w in w_refs]
    width = values[0].shape[1]
    for t, value in enumerate(values):
        @pl.when((h == 0) & (h < SPLIT - 1))
        def _():
            acc_ref[t] = value

        @pl.when((h > 0) & (h < SPLIT - 1))
        def _():
            acc_ref[t] += value

        @pl.when(h == SPLIT - 1)
        def _():
            total = (value if SPLIT == 1 else acc_ref[t] + value).astype(BF16)
            for j in range(count):
                @pl.when(k == j)
                def _():
                    out_refs[j][:, t * width:(t + 1) * width] = total


def partial_parts(act, ws, my_row, n_row, transposed):
    dims = NT if transposed else NN
    hidden_axis = 0 if transposed else 1
    width = ws[0].shape[hidden_axis] // n_row
    tokens, features = act.shape
    if not use_kernels(width, features):
        fulls = [mm(act, w, dims).astype(BF16) for w in ws]
        return [
            jnp.concatenate(
                [lax.dynamic_slice_in_dim(f, (my_row ^ k) * width, width, 1) for f in fulls], axis=1)
            for k in range(n_row)
        ]
    piece = features // SPLIT
    if transposed:
        w_spec = pl.BlockSpec((width, piece), lambda k, h, r: (r[0] ^ k, h))
    else:
        w_spec = pl.BlockSpec((piece, width), lambda k, h, r: (h, r[0] ^ k))
    part = jax.ShapeDtypeStruct((tokens, width * len(ws)), BF16)
    return pl.pallas_call(
        functools.partial(parts_kernel, dims, n_row, len(ws)),
        grid_spec=pltpu.PrefetchScalarGridSpec(
            num_scalar_prefetch=1,
            grid=(n_row, SPLIT),
            in_specs=[pl.BlockSpec((tokens, piece), lambda k, h, r: (0, h))] + [w_spec] * len(ws),
            out_specs=[whole_block(part.shape)] * n_row,
            scratch_shapes=[pltpu.VMEM((len(ws), tokens, width), F32)],
        ),
        out_shape=[part] * n_row,
        compiler_params=params(),
        cost_estimate=cost(2 * tokens * ws[0].size * len(ws), act, *ws),
        name="partial_parts",
    )(my_row.reshape(1), act, *ws)


def branch_kernel(count, pieces, row_ref, *refs):
    grads, (wg_ref, wu_ref) = refs[:count], refs[count:count + 2]
    outs, acc_ref = refs[count + 2:count + 2 + pieces], refs[-1]
    k, h = pl.program_id(0), pl.program_id(1)
    width = wg_ref.shape[1]
    for j in range(count):
        @pl.when(k == j)
        def _():
            value = mm(grads[j][:, :width], wg_ref[...], NT) + mm(grads[j][:, width:], wu_ref[...], NT)
            acc_ref[h] = value if j == 0 else acc_ref[h] + value

    @pl.when(k == count - 1)
    def _():
        rows = acc_ref.shape[1] // pieces
        cols = acc_ref.shape[2]
        for i in range(SPLIT):
            @pl.when(h == i)
            def _():
                for j in range(pieces):
                    outs[j][:, i * cols:(i + 1) * cols] = (
                        acc_ref[i, j * rows:(j + 1) * rows, :].astype(BF16))


def branch_parts(grads, w_gate, w_up, my_row, n_row, n_col):
    tokens, width = grads[0].shape[0], grads[0].shape[1] // 2
    rows, features = tokens // n_col, w_gate.shape[0]
    if not use_kernels(width, features):
        full = mm(place([g[:, :width] for g in grads], my_row), w_gate, NT)
        full = full + mm(place([g[:, width:] for g in grads], my_row), w_up, NT)
        full = full.astype(BF16)
        return [full[j * rows:(j + 1) * rows] for j in range(n_col)]
    part = jax.ShapeDtypeStruct((rows, features), BF16)
    piece = features // SPLIT
    w_spec = pl.BlockSpec((piece, width), lambda k, h, r: (h, r[0] ^ k))
    return pl.pallas_call(
        functools.partial(branch_kernel, n_row, n_col),
        grid_spec=pltpu.PrefetchScalarGridSpec(
            num_scalar_prefetch=1,
            grid=(n_row, SPLIT),
            in_specs=[whole_block(grads[0].shape)] * n_row + [w_spec, w_spec],
            out_specs=[whole_block(part.shape)] * n_col,
            scratch_shapes=[pltpu.VMEM((SPLIT, tokens, piece), F32)],
        ),
        out_shape=[part] * n_col,
        compiler_params=params(),
        cost_estimate=cost(4 * tokens * w_gate.size, w_gate, w_up),
        name="branch_parts",
    )(my_row.reshape(1), *grads, w_gate, w_up)


def grad_kernel(count, hidden_first, info_ref, act_ref, *refs):
    news, olds, out_ref = refs[:count], refs[count:-1], refs[-1]
    k = pl.program_id(0)

    def run(part_ref):
        if hidden_first:
            out_ref[...] = mm(part_ref[...], act_ref[...], TN)
        else:
            out_ref[...] = mm(act_ref[...], part_ref[...], TN)

    for j in range(count):
        if not olds:
            pl.when(k == j)(functools.partial(run, news[j]))
        else:
            fresh = info_ref[1] == 1
            pl.when((k == j) & fresh)(functools.partial(run, news[j]))
            pl.when((k == j) & jnp.logical_not(fresh))(functools.partial(run, olds[j]))


def weight_grad(act, news, olds, my_row, is_fresh, slot, slots, hidden_first, name):
    count = len(news)
    tokens, width = news[0].shape[0], news[0].shape[1] // slots
    features = act.shape[1]
    if not use_kernels(width, features):
        if olds:
            news = [jnp.where(is_fresh, a, b) for a, b in zip(news, olds)]
        hidden = place([a[:, slot * width:(slot + 1) * width] for a in news], my_row)
        return mm(hidden, act, TN) if hidden_first else mm(act, hidden, TN)
    piece = features // SPLIT
    if hidden_first:
        out = jax.ShapeDtypeStruct((width * count, features), F32)
        out_spec = pl.BlockSpec((width, piece), lambda k, h, r: (r[0] ^ k, h))
    else:
        out = jax.ShapeDtypeStruct((features, width * count), F32)
        out_spec = pl.BlockSpec((piece, width), lambda k, h, r: (h, r[0] ^ k))
    info = jnp.stack([my_row, is_fresh.astype(jnp.int32)])
    part_spec = pl.BlockSpec((tokens, width), lambda k, h, r: (0, slot))
    return pl.pallas_call(
        functools.partial(grad_kernel, count, hidden_first),
        grid_spec=pltpu.PrefetchScalarGridSpec(
            num_scalar_prefetch=1,
            grid=(count, SPLIT),
            in_specs=[pl.BlockSpec((tokens, piece), lambda k, h, r: (0, h))]
            + [part_spec] * (count + len(olds)),
            out_specs=out_spec,
        ),
        out_shape=out,
        compiler_params=params(),
        cost_estimate=cost(2 * tokens * features * width * count, out),
        name=name,
    )(info, act, *news, *olds)


def row_swap(block, k, sections):
    n_row = lax.axis_size("row")
    pairs = [(s * n_row + i, s * n_row + (i ^ k)) for s in sections for i in range(n_row)]
    return lax.ppermute(block, ("section", "row"), pairs)


def col_shift(block, k, section_step=0):
    n_sections, n_col = lax.axis_size("section"), lax.axis_size("col")
    pairs = [
        (s * n_col + i, (s + section_step) % n_sections * n_col + (i + k) % n_col)
        for s in range(n_sections)
        for i in range(n_col)
    ]
    return lax.ppermute(block, ("section", "col"), pairs)


def row_collect(parts, sections):
    return [parts[0]] + [row_swap(parts[k], k, sections) for k in range(1, len(parts))]


def row_spread(own, sections):
    return [own] + [row_swap(own, k, sections) for k in range(1, lax.axis_size("row"))]


def total_of(blocks):
    return sum(block.astype(F32) for block in blocks)


def shards(section_inputs, out_grad, gate_weight, up_weight, down_weight):
    section_id = lax.axis_index("section")
    my_row = lax.axis_index("row").astype(jnp.int32)
    n_sections, n_row, n_col = (lax.axis_size(a) for a in ("section", "row", "col"))
    everyone = range(n_sections)
    w_gate, w_up, w_down = gate_weight[0], up_weight[0], down_weight[0]
    merged_shape = (section_inputs.shape[1] * section_inputs.shape[2], section_inputs.shape[3])
    features = merged_shape[1]
    x_local = section_inputs[0].reshape(merged_shape)
    dy_local = out_grad.reshape(merged_shape)
    last = n_sections - 1
    is_fresh = section_id == 0

    pair = jnp.concatenate([x_local, dy_local], axis=1)
    both = jnp.concatenate([pair] + [col_shift(pair, k) for k in range(1, n_col)], axis=0)
    x_whole, dy_whole = both[:, :features], both[:, features:]
    wide_parts = partial_parts(x_whole, [w_gate, w_up], my_row, n_row, False)
    wide = row_collect(wide_parts, everyone)
    width = wide[0].shape[1] // 2
    gate = total_of([w[:, :width] for w in wide])
    up = total_of([w[:, width:] for w in wide])
    sigmoid_gate = jax.nn.sigmoid(gate)
    activated = gate * sigmoid_gate
    slope = sigmoid_gate * (1.0 + gate * (1.0 - sigmoid_gate))
    hidden = (activated * up).astype(BF16)

    input_grad = dy_local
    result = None
    olds = []
    for step in range(n_sections):
        active = last - step
        is_active = section_id == active
        if step:
            arrived = [col_shift(input_grad, k, -1) for k in range(n_col)]
            dy_local = jnp.where(is_active, arrived[0], dy_local)
            dy_whole = jnp.where(is_active, jnp.concatenate(arrived, axis=0), dy_whole)
        down_parts = partial_parts(dy_whole, [w_down], my_row, n_row, True)
        down = row_collect(down_parts, [active] if step == 0 else everyone)
        if step == last:
            grad_down = weight_grad(dy_whole, hiddens, [], my_row, is_fresh, 0, 1, True, "grad_down")
            down, grad_down = lax.optimization_barrier((down, grad_down))
        hidden_grad = total_of(down)
        both_grad = jnp.concatenate(
            [(hidden_grad * up * slope).astype(BF16), (hidden_grad * activated).astype(BF16)], axis=1)
        news = row_spread(both_grad, [active])
        if step == 0:
            hidden, news = lax.optimization_barrier((hidden, news))
            hiddens = row_spread(hidden, everyone)
        pieces = branch_parts(news, w_gate, w_up, my_row, n_row, n_col)
        total = total_of([pieces[0]] + [col_shift(pieces[k], -k) for k in range(1, n_col)])
        input_grad = (dy_local.astype(F32) + total).astype(BF16)
        result = input_grad if result is None else jnp.where(is_active, input_grad, result)
        if step < last:
            olds = [jnp.where(is_active, a, b) for a, b in zip(news, olds)] if olds else news

    grad_gate = weight_grad(x_whole, news, olds, my_row, is_fresh, 0, 2, False, "grad_gate")
    grad_up = weight_grad(x_whole, news, olds, my_row, is_fresh, 1, 2, False, "grad_up")
    return (
        result.reshape(section_inputs.shape),
        grad_gate[None],
        grad_up[None],
        grad_down[None],
    )


def solution(mesh):
    return jax.shard_map(
        shards,
        mesh=mesh,
        in_specs=(
            P("section", None, "col", "row"),
            P(None, "col", "row"),
            P("section", "row", "col"),
            P("section", "row", "col"),
            P("section", "col", "row"),
        ),
        out_specs=(
            P("section", None, "col", "row"),
            P("section", "row", "col"),
            P("section", "row", "col"),
            P("section", "col", "row"),
        ),
        check_vma=False,
    )
```
